32 devices in a mesh: groups: 2 (over y), lon: 16 (over z, x, core).
Axes of the slice: x: 2, y: 2, z: 4, core: 2. Of those that a mesh axis runs over, the one named last changes fastest.
Arguments:
- fields: bfloat16 [4, 24, 192, 192], P('groups', None, 'lon'), parts along dimension 0, may hold values from -6 to 6
- norm_gain: float32 [192], replicated, may hold values from 0.25 to 1.75
- qkv_weight: bfloat16 [192, 576], replicated, may hold values from -2.5 to 2.5
- proj_weight: bfloat16 [192, 192], replicated, may hold values from -0.4375 to 0.4375
- bias_table: float32 [4, 6, 3312], replicated, may hold values from -4 to 4
- bias_index: int32 [144, 144], replicated, may hold values from 0 to 3311
- region_ids: int32 [2, 24], replicated, may hold values from 0 to 2
- mlp_gain: float32 [192], replicated, may hold values from 0.25 to 1.75
- up_weight: bfloat16 [192, 768], replicated, may hold values from -0.4375 to 0.4375
- down_weight: bfloat16 [768, 192], replicated, may hold values from -0.21875 to 0.21875
- merge_gain: float32 [768], replicated, may hold values from 0.25 to 1.75
- merge_weight: bfloat16 [768, 384], replicated, may hold values from -0.21875 to 0.21875
- cotangent: bfloat16 [4, 12, 96, 384], P('groups', None, 'lon'), parts along dimension 0, may hold values from -12 to 12
Outputs:
- merged: bfloat16 [4, 12, 96, 384], P('groups', None, 'lon'), parts along dimension 0
- field_grad: bfloat16 [4, 24, 192, 192], P('groups', None, 'lon'), parts along dimension 0
- qkv_grad: float32 [384, 576], P('groups'), parts along dimension 0
- proj_grad: float32 [384, 192], P('groups'), parts along dimension 0
- up_grad: float32 [384, 768], P('groups'), parts along dimension 0
- down_grad: float32 [1536, 192], P('groups'), parts along dimension 0
- merge_grad: float32 [1536, 384], P('groups'), parts along dimension 0
- table_grad: float32 [8, 6, 3312], P('groups'), parts along dimension 0
The draws below stay inside these ranges and needn't reach their ends.
There are 2 independent parts, one for each index of `groups`. The reference program is written for one: setup_inputs(seed, part) draws one part's arguments, and reference() takes and returns one part's arrays. A program takes and returns all parts, laid end to end along the dimension named above; an argument that names none is the same for every part. Nothing has to cross between parts.
All inputs are finite; a program needn't handle non-finite values.
Results may differ from the reference program's by a relative error of at most 0.019.
The reference program's roundings to bfloat16 on the way count: a program that leaves them out, or rounds other values in their place, can miss the bound.
Values may be sent and summed in bfloat16 or wider, within the bound.
A program may use at most 192 MiB of HBM per device.

```python
import jax
import jax.numpy as jnp
from jax import lax

C = 192
MLP = 768
HEADS = 6
HEAD = 32
WZ = 2
WLAT = 6
WLON = 12
HALF = 6
WIN = 144
BPOS = 3312
Z = 2
LAT = 24
NLON = 192
TYPES = 4


def draw_qkv_weight(key, part):
    entries = jnp.clip(jax.random.normal(key, (C, 3 * C), jnp.float32), -6.0, 6.0) * C ** (-0.5)
    entries = jnp.clip(entries, -2.5, 2.5)
    return entries.astype(jnp.bfloat16)


def draw_cotangent(key, part):
    dims_full = (Z, LAT // 2, NLON // 2, 2 * C)
    position = jnp.arange(NLON // 2).astype(jnp.float32) / (NLON // 2)
    rising = jnp.exp(jnp.log(3.0) * position)[None, None, :, None]
    noise_part = jnp.clip(jax.random.normal(key, dims_full, jnp.float32), -4.0, 4.0)
    return (noise_part * rising).astype(jnp.bfloat16)


def set_ends(array, stream_key, least, top_value):
    longest = array.shape.index(max(array.shape))
    spots = []
    for shift in (0, 1):
        where = [jax.random.randint(jax.random.fold_in(stream_key, axis), (), 0, length) for axis, length in enumerate(array.shape)]
        where[longest] = (where[longest] + shift) % array.shape[longest]
        spots.append(tuple(where))
    return array.at[spots[0]].set(least).at[spots[1]].set(top_value)


def steps_of(rng, shape, shards, least, top_value):
    gain = 1.0
    for dim, blocks in shards:
        draws = jax.random.uniform(jax.random.fold_in(jax.random.fold_in(rng, 6), dim), (blocks,), jnp.float32, least / len(shards), top_value / len(shards))
        gain = gain * jnp.repeat(jnp.exp(draws), shape[dim] // blocks).reshape((-1,) + (1,) * (len(shape) - 1 - dim))
    return gain


def bell_draw(rng, shape, scale, most, cuts=(), dtype=jnp.bfloat16):
    drawn = jax.random.normal(rng, shape, jnp.float32) * scale
    if len(cuts) > 0:
        drawn = steps_of(rng, shape, cuts, -0.22, 0.18) * drawn
    return jnp.clip(drawn, min=-most, max=most).astype(dtype)


def setup_inputs(seed: int = 0, part: int = 0) -> dict:
    streams_of = jax.random.split(jax.random.key(seed), 14)
    part_splits = jax.random.split(jax.random.fold_in(streams_of[13], part), 14)
    fields = bell_draw(part_splits[0], (Z, LAT, NLON, C), 1.0, 6.0, ((2, 16),))
    norm_gain = jnp.clip(1.0 + 0.15 * jax.random.normal(streams_of[1], (C,), jnp.float32), 0.25, 1.75)
    qkv_weight = draw_qkv_weight(jax.random.fold_in(streams_of[13], 71), part)
    proj_weight = bell_draw(streams_of[3], (C, C), C ** -0.5, 0.4375)
    bias_table = bell_draw(streams_of[4], (TYPES, HEADS, BPOS), 1.0, 4.0, (), jnp.float32)
    bias_index = set_ends(jax.random.randint(streams_of[5], (WIN, WIN), 0, BPOS), jax.random.fold_in(streams_of[5], 1), 0, BPOS - 1).astype(jnp.int32)
    region_ids = set_ends(jax.random.randint(streams_of[6], (Z, LAT), 0, 3), jax.random.fold_in(streams_of[6], 1), 0, 2).astype(jnp.int32)
    mlp_gain = jnp.clip(1.0 + 0.15 * jax.random.normal(streams_of[7], (C,), jnp.float32), 0.25, 1.75)
    up_weight = bell_draw(streams_of[8], (C, MLP), C ** -0.5, 0.4375)
    down_weight = bell_draw(streams_of[9], (MLP, C), MLP ** -0.5, 0.21875)
    merge_gain = jnp.clip(1.0 + 0.15 * jax.random.normal(streams_of[10], (4 * C,), jnp.float32), 0.25, 1.75)
    merge_weight = bell_draw(streams_of[11], (4 * C, 2 * C), (4 * C) ** -0.5, 0.21875)
    cotangent = draw_cotangent(jax.random.fold_in(jax.random.fold_in(streams_of[13], part), 71), part)
    return {"fields": fields, "norm_gain": norm_gain, "qkv_weight": qkv_weight, "proj_weight": proj_weight, "bias_table": bias_table, "bias_index": bias_index, "region_ids": region_ids, "mlp_gain": mlp_gain, "up_weight": up_weight, "down_weight": down_weight, "merge_gain": merge_gain, "merge_weight": merge_weight, "cotangent": cotangent}


def layer_norm(values, norm_gain):
    average = lax.optimization_barrier(jnp.mean(values, axis=-1, keepdims=True))
    centred = values - average
    variance = lax.optimization_barrier(jnp.mean(centred * centred, axis=-1, keepdims=True))
    return centred * lax.rsqrt(variance + 1e-05) * norm_gain

def to_windows(grid_in):
    levels, latitudes, longitudes, features = grid_in.shape
    blocks = grid_in.reshape(levels // WZ, WZ, latitudes // WLAT, WLAT, longitudes // WLON, WLON, features)
    blocks = blocks.transpose(0, 2, 4, 1, 3, 5, 6)
    return blocks.reshape(levels // WZ * (latitudes // WLAT), longitudes // WLON, WIN, features)

def from_windows(windows, levels, latitudes):
    number = windows.shape[1]
    features = windows.shape[3]
    blocks = windows.reshape(levels // WZ, latitudes // WLAT, number, WZ, WLAT, WLON, features)
    blocks = blocks.transpose(0, 3, 1, 4, 2, 5, 6)
    return blocks.reshape(levels, latitudes, number * WLON, features)

def region_mask(region_ids):
    labels = region_ids.reshape(Z // WZ, WZ, LAT // WLAT, WLAT).transpose(0, 2, 1, 3)
    labels = jnp.repeat(labels.reshape(TYPES, WZ * WLAT), WLON, axis=1)
    return labels[:, :, None] == labels[:, None, :]

def regroup(grid_in):
    levels, latitudes, longitudes, features = grid_in.shape
    blocks = grid_in.reshape(levels, latitudes // 2, 2, longitudes // 2, 2, features)
    return blocks.transpose(0, 1, 3, 2, 4, 5).reshape(levels, latitudes // 2, longitudes // 2, 4 * features)

def attend_one(tokens_win, qkv_weight, proj_weight, bias_rows, same_region, probe_qkv, probe_proj):
    triple = (jnp.dot(tokens_win, qkv_weight, preferred_element_type=jnp.float32) + probe_qkv).astype(jnp.bfloat16)
    shaped = triple.reshape(tokens_win.shape[:2] + (3, HEADS, HEAD)).astype(jnp.float32)
    scores = jnp.einsum('wqhd,wkhd->whqk', shaped[:, :, 0], shaped[:, :, 1]) * HEAD ** (-0.5) + bias_rows
    scores = jnp.where(same_region, scores, -1e+30)
    row_max = lax.optimization_barrier(jnp.max(scores, axis=-1, keepdims=True))
    weights = jnp.exp(scores - row_max)
    probability = (weights / lax.optimization_barrier(jnp.sum(weights, axis=-1, keepdims=True))).astype(jnp.bfloat16)
    mixed_heads = jnp.einsum('whqk,wkhd->wqhd', probability.astype(jnp.float32), shaped[:, :, 2])
    mixed_heads = mixed_heads.astype(jnp.bfloat16).reshape(tokens_win.shape)
    result = jnp.dot(mixed_heads, proj_weight, preferred_element_type=jnp.float32) + probe_proj
    return (result.astype(jnp.bfloat16), mixed_heads)

def weight_term(inputs, grads):
    rows_in = inputs.reshape(-1, inputs.shape[-1])
    rows_out = grads.reshape(-1, grads.shape[-1]).astype(jnp.bfloat16)
    return jnp.dot(rows_in.T, rows_out, preferred_element_type=jnp.float32)

def table_sums(grad_bias, bias_index):
    flat = grad_bias.reshape(TYPES * HEADS, WIN * WIN).T
    summed = jax.ops.segment_sum(flat, bias_index.reshape(-1), num_segments=BPOS)
    return summed.T.reshape(TYPES, HEADS, BPOS)

def reference(fields, norm_gain, qkv_weight, proj_weight, bias_table, bias_index, region_ids, mlp_gain, up_weight, down_weight, merge_gain, merge_weight, cotangent):
    same_region = region_mask(region_ids)
    bias_rows = jnp.take(bias_table, bias_index, axis=2)

    def forward(fields_in, bias_in, probes):
        probe_qkv, probe_proj, probe_up, probe_down, probe_merge = probes
        field_f32 = fields_in.astype(jnp.float32)
        normed = layer_norm(field_f32, norm_gain).astype(jnp.bfloat16)
        rolled = jnp.roll(normed, -HALF, axis=2)
        tokens_win = to_windows(rolled)

        def per_type(parts):
            return attend_one(parts[0], qkv_weight, proj_weight, parts[1][None], parts[2], parts[3], parts[4])
        result, mixed_heads = lax.map(jax.checkpoint(per_type), (tokens_win, bias_in, same_region, probe_qkv, probe_proj))
        branch = jnp.roll(from_windows(result, Z, LAT), HALF, axis=2)
        after_attn = lax.optimization_barrier((field_f32 + branch.astype(jnp.float32)).astype(jnp.bfloat16))
        after_f32 = after_attn.astype(jnp.float32)
        normed_mlp = layer_norm(after_f32, mlp_gain).astype(jnp.bfloat16)
        hidden = jax.nn.gelu(jnp.dot(normed_mlp, up_weight, preferred_element_type=jnp.float32) + probe_up, approximate=False).astype(jnp.bfloat16)
        after_mlp = (after_f32 + jnp.dot(hidden, down_weight, preferred_element_type=jnp.float32) + probe_down).astype(jnp.bfloat16)
        normed_merge = layer_norm(regroup(after_mlp).astype(jnp.float32), merge_gain).astype(jnp.bfloat16)
        merged = (jnp.dot(normed_merge, merge_weight, preferred_element_type=jnp.float32) + probe_merge).astype(jnp.bfloat16)
        return (merged, (tokens_win, mixed_heads, normed_mlp, hidden, normed_merge))
    windows_lon = NLON // WLON
    probes = (jnp.zeros((TYPES, windows_lon, WIN, 3 * C), jnp.float32), jnp.zeros((TYPES, windows_lon, WIN, C), jnp.float32), jnp.zeros((Z, LAT, NLON, MLP), jnp.float32), jnp.zeros((Z, LAT, NLON, C), jnp.float32), jnp.zeros((Z, LAT // 2, NLON // 2, 2 * C), jnp.float32))
    merged, backward, stored = jax.vjp(forward, fields, bias_rows, probes, has_aux=True)
    field_grad, grad_bias, grad_probes = backward(cotangent)
    tokens_win, mixed_heads, normed_mlp, hidden, normed_merge = stored
    grad_qkv, grad_proj, grad_up, grad_down, grad_merge = grad_probes
    factor = float(Z * LAT * NLON) ** (-0.5)
    qkv_grad = weight_term(tokens_win, grad_qkv) * factor
    proj_grad = weight_term(mixed_heads, grad_proj) * factor
    up_grad = weight_term(normed_mlp, grad_up) * factor
    down_grad = weight_term(hidden, grad_down) * factor
    merge_grad = weight_term(normed_merge, grad_merge) * factor
    table_grad = table_sums(grad_bias, bias_index) * factor
    return (merged, field_grad, qkv_grad, proj_grad, up_grad, down_grad, merge_grad, table_grad)
```

```python
import functools

import jax
import jax.numpy as jnp
import numpy as np
from jax import lax
from jax.experimental import pallas as pl
from jax.experimental.pallas import tpu as pltpu
from jax.sharding import PartitionSpec as P

C = 192
MLP = 768
HEADS = 6
HEAD = 32
WZ = 2
WLAT = 6
WLON = 12
HALF = 6
WIN = 144
BPOS = 3312
Z = 2
LAT = 24
TYPES = 4
TH = TYPES * HEADS
LANES = 128
RADIX = 256
DIGITS = -(-BPOS // RADIX)
GROUP = WIN // 4
GPAD = 48
TAIL = WIN - LANES
WIDE = (HEADS + 1) * LANES
TOK = TYPES * WIN
UNROLL = 4
ROWS = (18 * LANES, 12 * C, 6 * C, 2 * DIGITS * TH)
BF = jnp.bfloat16
F32 = jnp.float32
VMEM = pl.BlockSpec(memory_space=pltpu.VMEM)
ANY = pl.BlockSpec(memory_space=pl.ANY)
NT = ((1,), (1,))
TN = ((0,), (0,))


def dot(a, b, dims=((1,), (0,))):
    return lax.dot_general(a, b, (dims, ((), ())), preferred_element_type=F32)


def norm_parts(values):
    average = jnp.mean(values, axis=-1, keepdims=True)
    centred = values - average
    variance = jnp.mean(centred * centred, axis=-1, keepdims=True)
    scale = lax.rsqrt(variance + 1e-05)
    return centred * scale, scale


def norm_grad(hat, scale, grad_hat):
    first = jnp.mean(grad_hat, axis=-1, keepdims=True)
    second = jnp.mean(grad_hat * hat, axis=-1, keepdims=True)
    return scale * (grad_hat - first - hat * second)


def grid_sides(n):
    chips = n // 2
    fast = 1
    while fast * fast * 8 <= chips:
        fast *= 2
    return chips // fast, fast


def piece_rows(n):
    step = 16 * n
    return [-(-rows // step) * step for rows in ROWS]


class Sum:
    def __init__(self, n, rows, packed, out, paired, half_sum, crossed, part_sum, landed, send, recv):
        self.slow, self.fast = grid_sides(n)
        self.share = rows // n
        me = lax.axis_index("lon")
        self.core = lax.rem(me, 2)
        self.x = lax.rem(me // 2, self.fast)
        self.z = me // (2 * self.fast)
        self.packed, self.out = packed, out
        self.paired, self.half_sum, self.crossed = paired, half_sum, crossed
        self.part_sum, self.landed = part_sum, landed
        self.send, self.recv = send, recv
        self.used = 0
        self.started = []

    def device(self, z, x, core):
        return (z * self.fast + x) * 2 + core

    def copy(self, src, dst, device):
        made = pltpu.make_async_remote_copy(
            src_ref=src, dst_ref=dst, send_sem=self.send.at[self.used],
            recv_sem=self.recv.at[self.used],
            device_id={"lon": device}, device_id_type=pl.DeviceIdType.MESH,
        )
        made.start()
        self.used += 1
        self.started.append(made)
        return made

    def at(self, index, count):
        return pl.ds(pl.multiple_of(index * self.share, 16), count * self.share)

    def across_x(self):
        return [lax.rem(self.x + k, self.fast) for k in range(1, self.fast)]

    def across_z(self):
        return [lax.rem(self.z + k, self.slow) for k in range(1, self.slow)]

    def s0(self):
        count = self.slow * self.fast
        other = 1 - self.core
        self.waits = [self.copy(
            self.packed.at[self.at(other * count, count), :], self.paired,
            self.device(self.z, self.x, other),
        )]

    def s1(self):
        count = self.slow * self.fast
        self.waits[0].wait_recv()
        mine = self.packed[self.at(self.core * count, count), :].astype(F32)
        self.half_sum[...] = (mine + self.paired[...].astype(F32)).astype(BF)
        self.waits = [
            self.copy(
                self.half_sum.at[self.at(x * self.slow, self.slow), :], self.crossed.at[k],
                self.device(self.z, x, self.core),
            )
            for k, x in enumerate(self.across_x())
        ]

    def s2(self):
        total = self.half_sum[self.at(self.x * self.slow, self.slow), :].astype(F32)
        for k, made in enumerate(self.waits):
            made.wait_recv()
            total = total + self.crossed[k].astype(F32)
        self.part_sum[...] = total.astype(BF)
        self.waits = [
            self.copy(
                self.part_sum.at[self.at(z, 1), :], self.landed.at[k],
                self.device(z, self.x, self.core),
            )
            for k, z in enumerate(self.across_z())
        ]

    def s3(self):
        total = self.part_sum[self.at(self.z, 1), :].astype(F32)
        for k, made in enumerate(self.waits):
            made.wait_recv()
            total = total + self.landed[k].astype(F32)
        rows = self.at((self.core * self.fast + self.x) * self.slow + self.z, 1)
        self.out[rows, :] = total.astype(BF)
        self.waits = [
            self.copy(
                self.out.at[rows, :], self.out.at[rows, :], self.device(z, self.x, self.core)
            )
            for z in self.across_z()
        ]

    def s4(self):
        for made in self.waits:
            made.wait_recv()
        rows = self.at((self.core * self.fast + self.x) * self.slow, self.slow)
        self.waits = [
            self.copy(
                self.out.at[rows, :], self.out.at[rows, :], self.device(self.z, x, self.core)
            )
            for x in self.across_x()
        ]

    def s5(self):
        for made in self.waits:
            made.wait_recv()
        count = self.slow * self.fast
        rows = self.at(self.core * count, count)
        self.waits = [self.copy(
            self.out.at[rows, :], self.out.at[rows, :], self.device(self.z, self.x, 1 - self.core)
        )]

    def s6(self):
        for made in self.waits:
            made.wait_recv()
        for made in self.started:
            made.wait_send()


def block_kernel(
    n,
    gains_ref, tail_index_ref, labels_ref, perm_ref,
    fields_hbm, ct_hbm, table_hbm, index_hbm, wqkv_hbm, wproj_hbm, wup_hbm, wdown_hbm, wm_hbm,
    merged_ref, fgrad_ref, out1, out2, out3, out4,
    fields, east, ct, east_ct, table, index, wqkv, wproj, wup, wdown, wm, in_sem,
    edge_send, edge_recv, merged_in, merged_out, fgrad_in, fgrad_out,
    packed1, packed2, packed3, packed4,
    paired1, paired2, paired3, paired4, half1, half2, half3, half4,
    crossed1, crossed2, crossed3, crossed4, part1, part2, part3, part4,
    landed1, landed2, landed3, landed4, send1, send2, send3, send4, recv1, recv2, recv3, recv4,
    index_main, rows_in, ct_rows, xs, cts, tab, wt, bias, tail0, tail1, tails, eye,
    kbd, vbd, vbd2, wide, prob, probb, dsb, dscore, dtail0, dtail1, dtails,
    triple_t, s_normed, s_mixed, s_after, s_nmlp, s_slope, s_hidden, s_dy, s_nm, s_ct, s_du,
    s_da, s_dm, s_dt, grad_rows, merged_rows, s_table,
):
    me = lax.axis_index("lon")
    east_of, west_of = lax.rem(me + 1, n), lax.rem(me + n - 1, n)
    rows_of = piece_rows(n)
    sums = [
        Sum(n, rows, *refs) for rows, *refs in zip(
            rows_of, (packed1, packed2, packed3, packed4), (out1, out2, out3, out4),
            (paired1, paired2, paired3, paired4), (half1, half2, half3, half4),
            (crossed1, crossed2, crossed3, crossed4), (part1, part2, part3, part4),
            (landed1, landed2, landed3, landed4), (send1, send2, send3, send4),
            (recv1, recv2, recv3, recv4),
        )
    ]
    first = sums[0]

    local_copies = []
    for k, (src, dst) in enumerate((
        (table_hbm, table), (index_hbm, index), (fields_hbm, fields), (wqkv_hbm, wqkv),
        (wproj_hbm, wproj), (wup_hbm, wup), (wdown_hbm, wdown), (wm_hbm, wm), (ct_hbm, ct),
    )):
        made = pltpu.make_async_copy(src, dst, in_sem.at[k])
        made.start()
        local_copies.append(made)

    peers = [first.device(first.z, first.x, 1 - first.core), west_of, east_of]
    peers += [first.device(first.z, x, first.core) for x in first.across_x()]
    peers += [first.device(z, first.x, first.core) for z in first.across_z()]
    barrier = pltpu.get_barrier_semaphore()
    for device in peers:
        pl.semaphore_signal(
            barrier, inc=1, device_id={"lon": device}, device_id_type=pl.DeviceIdType.MESH
        )
    pl.semaphore_wait(barrier, len(peers))

    def edge(k, src, dst, device):
        made = pltpu.make_async_remote_copy(
            src_ref=src, dst_ref=dst, send_sem=edge_send.at[k], recv_sem=edge_recv.at[k],
            device_id={"lon": device}, device_id_type=pl.DeviceIdType.MESH,
        )
        made.start()
        return made

    edges = [
        edge(0, fields_hbm.at[:, :, 0:8, :], east, west_of),
        edge(1, ct_hbm, east_ct, west_of),
    ]

    for ref in (tab, kbd, vbd, vbd2, cts, dtails, tails):
        ref[...] = jnp.zeros_like(ref)
    eye[...] = (
        lax.broadcasted_iota(jnp.int32, (C, C), 0) == lax.broadcasted_iota(jnp.int32, (C, C), 1)
    ).astype(BF)

    local_copies[0].wait()
    for d in range(DIGITS):
        width = min(RADIX, BPOS - d * RADIX)
        for t in range(TYPES):
            start = d * TH + t * HEADS
            tab[start:start + HEADS, :width] = table[t, :, d * RADIX:d * RADIX + width]
    local_copies[1].wait()
    index_main[...] = index[:, 0:LANES]

    def position_of(where):
        digit = where >> 8
        lane = jnp.where(where < 0, -1, where & (RADIX - 1))
        hot = (lax.broadcasted_iota(jnp.int32, (RADIX, RADIX), 0) == lane).astype(BF)
        return digit, hot

    def main_position(pair):
        return position_of(jnp.concatenate(
            [index_main[pl.ds(2 * pair, 1), :], index_main[pl.ds(2 * pair + 1, 1), :]], axis=1
        ))

    def tail_position(key):
        return position_of(tail_index_ref[pl.ds(key, 1), :])

    table_bf = tab[...].astype(BF)
    tab_bf = dsb
    tab_bf[0:DIGITS * TH, 0:RADIX] = table_bf

    def looked_up(digit, hot):
        found = dot(tab_bf[0:DIGITS * TH, 0:RADIX], hot)
        total = jnp.zeros((TH, RADIX), F32)
        for d in range(DIGITS):
            total = jnp.where(digit == d, found[d * TH:(d + 1) * TH], total)
        return total

    def th_rows(i):
        return pl.ds(pl.multiple_of(i * TH, 8), TH)

    def main_bias(step, carry):
        for u in range(UNROLL):
            pair = step * UNROLL + u
            total = looked_up(*main_position(pair))
            bias[th_rows(2 * pair), :] = total[:, :LANES]
            bias[th_rows(2 * pair + 1), :] = total[:, LANES:]
        return carry

    lax.fori_loop(0, WIN // 2 // UNROLL, main_bias, 0)

    def tail_bias(step, carry):
        for u in range(UNROLL):
            key = step * UNROLL + u
            total = looked_up(*tail_position(key))
            tail0[th_rows(key), :] = total[:, :LANES]
            tail1[th_rows(key), :] = total[:, LANES:]
        return carry

    lax.fori_loop(0, TAIL // UNROLL, tail_bias, 0)

    for made in local_copies[2:4]:
        made.wait()
    wt[...] = dot(wqkv[...], eye[...], TN).astype(BF)
    edges[0].wait_recv()
    for z in range(Z):
        for a in range(LAT):
            k = z * LAT + a
            base = (a // WLAT) * WIN + z * WLAT * WLON + (a % WLAT) * WLON
            rows_in[16 * k:16 * k + WLON, :] = fields[z, a].astype(F32)
            xs[base:base + HALF, :] = rows_in[16 * k + HALF:16 * k + WLON, :]
    for z in range(Z):
        for a in range(LAT):
            k = z * LAT + a
            base = (a // WLAT) * WIN + z * WLAT * WLON + (a % WLAT) * WLON
            rows_in[16 * k:16 * k + 8, :] = east[z, a].astype(F32)
            xs[base + HALF:base + WLON, :] = rows_in[16 * k:16 * k + HALF, :]
    for made in local_copies[4:]:
        made.wait()
    edges[1].wait_recv()
    for part, ref in enumerate((ct, east_ct)):
        for z in range(Z):
            for a in range(LAT // 2):
                k = z * (LAT // 2) + a
                t, b = a // (WLAT // 2), a % (WLAT // 2)
                base = t * GPAD + z * (GROUP // 2) + b * HALF + part * (HALF // 2)
                ct_rows[8 * k:8 * k + HALF, :] = ref[z, a].astype(F32)
                skip = (1 - part) * (HALF // 2)
                cts[base:base + HALF // 2, :] = ct_rows[8 * k + skip:8 * k + skip + HALF // 2, :]
    s_ct[...] = cts[...].astype(BF)

    root = float(HEAD) ** (-0.5)
    low = -1e30
    lanes = lax.broadcasted_iota(jnp.int32, (1, LANES), 1)
    segs = [(lanes >= h * TAIL) & (lanes < (h + 1) * TAIL) for h in range(HEADS)]
    g1, g2 = gains_ref[0:1, :], gains_ref[1:2, :]

    def head_cols(h):
        return slice(h * LANES, (h + 1) * LANES)

    def place(dst, value_t):
        for h in range(HEADS):
            own = slice(h * HEAD, (h + 1) * HEAD)
            dst[own, head_cols(h)] = value_t[own, 0:LANES]
            at = HEADS * LANES + h * TAIL
            dst[own, at:at + TAIL] = value_t[own, LANES:WIN]

    def forward(t, carry):
        rows = pl.ds(pl.multiple_of(t * WIN, 16), WIN)
        field = xs[rows, :]
        hat1, _ = norm_parts(field)
        normed = (hat1 * g1).astype(BF)
        s_normed[rows, :] = normed
        triple_t[t] = dot(wt[...], normed, NT).astype(BF)
        q = dot(normed, wqkv[:, 0:C]).astype(BF)
        v = dot(normed, wqkv[:, 2 * C:3 * C]).astype(BF)
        place(kbd, triple_t.at[t, C:2 * C])
        for h in range(HEADS):
            own = slice(h * HEAD, (h + 1) * HEAD)
            vbd2[head_cols(h), own] = v[0:LANES, own]
            at = HEADS * LANES + h * TAIL
            vbd2[at:at + TAIL, own] = v[LANES:WIN, own]
        wide[...] = dot(q, kbd[...])

        label_q = labels_ref[pl.ds(t, 1), :]
        label_k = labels_ref[pl.ds(TYPES + t, 1), :]
        ids = lax.broadcasted_iota(jnp.int32, (8, RADIX), 0)
        same = dot((ids == label_q).astype(BF), (ids == label_k).astype(BF), TN)[0:WIN] > 0.5
        same_main, same_tail = same[:, :LANES], same[:, LANES:]

        for h in range(HEADS):
            picked = pl.ds(t * HEADS + h, TAIL, stride=TH)
            tails[h * TAIL:(h + 1) * TAIL, 0:LANES] = tail0[picked, :]
            tails[h * TAIL:(h + 1) * TAIL, LANES:] = tail1[picked, :]
        tail_bias_t = jnp.transpose(tails[...])[0:WIN]
        s_tail = jnp.where(same_tail, wide[:, HEADS * LANES:] * root + tail_bias_t, low)
        top_tail = jnp.zeros((WIN, LANES), F32)
        for h in range(HEADS):
            picked = pl.ds(t * HEADS + h, WIN, stride=TH)
            s = jnp.where(same_main, wide[:, head_cols(h)] * root + bias[picked, :], low)
            top = jnp.max(jnp.maximum(s, jnp.where(segs[h], s_tail, low)), axis=-1, keepdims=True)
            prob[t, :, head_cols(h)] = jnp.exp(s - top)
            top_tail = jnp.where(segs[h], top, top_tail)
        e_tail = jnp.exp(s_tail - top_tail)
        over_tail = jnp.zeros((WIN, LANES), F32)
        for h in range(HEADS):
            e = prob[t, :, head_cols(h)]
            over = 1.0 / jnp.sum(e + jnp.where(segs[h], e_tail, 0.0), axis=-1, keepdims=True)
            p = e * over
            prob[t, :, head_cols(h)] = p
            probb[t, :, head_cols(h)] = p.astype(BF)
            over_tail = jnp.where(segs[h], over, over_tail)
        p_tail = e_tail * over_tail
        prob[t, :, HEADS * LANES:] = p_tail
        probb[t, :, HEADS * LANES:] = p_tail.astype(BF)

        mixed = dot(probb[t], vbd2[...]).astype(BF)
        s_mixed[rows, :] = mixed
        branch = dot(mixed, wproj[...]).astype(BF).astype(F32)
        after_bf = (field + branch).astype(BF)
        s_after[rows, :] = after_bf
        after = after_bf.astype(F32)
        hat2, _ = norm_parts(after)
        nmlp = (hat2 * g2).astype(BF)
        s_nmlp[rows, :] = nmlp
        up = dot(nmlp, wup[...])
        cdf = 0.5 * (1.0 + lax.erf(up * np.float32(np.sqrt(0.5))))
        s_slope[rows, :] = cdf + up * (jnp.exp(-0.5 * up * up) * np.float32(1 / np.sqrt(2 * np.pi)))
        hidden = (up * cdf).astype(BF)
        s_hidden[rows, :] = hidden
        after_mlp = (after + dot(hidden, wdown[...])).astype(BF)

        spread = dot(perm_ref[...], after_mlp)
        parts = [spread[g * GPAD:(g + 1) * GPAD] for g in range(4)]
        average = sum(jnp.sum(p, axis=-1, keepdims=True) for p in parts) / (4 * C)
        parts = [p - average for p in parts]
        variance = sum(jnp.sum(p * p, axis=-1, keepdims=True) for p in parts) / (4 * C)
        scale = lax.rsqrt(variance + 1e-05)
        hats = [p * scale for p in parts]
        few = pl.ds(pl.multiple_of(t * GPAD, 16), GPAD)
        ct_t = s_ct[few, :]
        merged = jnp.zeros((GPAD, 2 * C), F32)
        grads = []
        for g in range(4):
            gain = gains_ref[2 + g:3 + g, :]
            weight = wm[g * C:(g + 1) * C, :]
            nm = (hats[g] * gain).astype(BF)
            s_nm[g, few, :] = nm
            merged = merged + dot(nm, weight)
            grads.append(dot(ct_t, weight, NT).astype(BF).astype(F32) * gain)
        merged_rows[few, :] = merged
        first = sum(jnp.sum(g, axis=-1, keepdims=True) for g in grads) / (4 * C)
        second = sum(
            jnp.sum(g * hat, axis=-1, keepdims=True) for g, hat in zip(grads, hats)
        ) / (4 * C)
        back = jnp.concatenate(
            [scale * (g - first - hat * second) for g, hat in zip(grads, hats)], axis=0
        ).astype(BF)
        s_dy[rows, :] = dot(perm_ref[...], back, TN).astype(BF)
        return carry

    lax.fori_loop(0, TYPES, forward, 0)

    def finish(packed, used):
        if packed.shape[0] > used:
            packed[used:, :] = jnp.zeros((packed.shape[0] - used, LANES), BF)

    for g in range(4):
        value = dot(s_nm[g], s_ct[...], TN)
        for b in range(3):
            packed1[b * 4 * C + g * C:b * 4 * C + (g + 1) * C, :] = (
                value[:, b * LANES:(b + 1) * LANES].astype(BF)
            )
    finish(packed1, ROWS[0])
    sums[0].s0()

    for z in range(Z):
        for a in range(LAT // 2):
            k = z * (LAT // 2) + a
            t, b = a // (WLAT // 2), a % (WLAT // 2)
            base = t * GPAD + z * (GROUP // 2) + b * HALF
            near, far = merged_rows[base:base + 3, :], merged_rows[base + 3:base + 6, :]
            ct_rows[8 * k + 3:8 * k + 6, :] = near
            cts[3 * k:3 * k + 3, :] = far
    merged_out[...] = cts[0:Z * LAT // 2 * 3, :].astype(BF)
    edges.append(edge(2, merged_out, merged_in, east_of))

    down = dot(s_hidden[...], s_dy[...], TN)
    packed2[0:MLP, :] = down[:, 0:LANES].astype(BF)
    packed2[MLP:MLP + MLP // 2, :] = jnp.concatenate(
        [down[0:MLP // 2, LANES:], down[MLP // 2:, LANES:]], axis=1
    ).astype(BF)
    sums[0].s1()

    def backward(t, carry):
        rows = pl.ds(pl.multiple_of(t * WIN, 16), WIN)
        dy = s_dy[rows, :]
        dhidden = dot(dy, wdown[...], NT).astype(BF).astype(F32)
        du = (dhidden * s_slope[rows, :]).astype(BF)
        s_du[rows, :] = du
        dn = dot(du, wup[...], NT).astype(BF).astype(F32) * g2
        hat2, scale2 = norm_parts(s_after[rows, :].astype(F32))
        da = (dy.astype(F32) + norm_grad(hat2, scale2, dn)).astype(BF)
        s_da[rows, :] = da
        return carry

    lax.fori_loop(0, TYPES, backward, 0)
    for b in range(6):
        value = dot(s_nmlp[...], s_du[:, b * LANES:(b + 1) * LANES], TN)
        start = 6 * C + b * C
        packed2[start:start + C, :] = value.astype(BF)
    finish(packed2, ROWS[1])
    sums[0].s2()
    sums[1].s0()

    def attend_back(t, carry):
        rows = pl.ds(pl.multiple_of(t * WIN, 16), WIN)
        da = s_da[rows, :]
        dm = dot(da, wproj[...], NT).astype(BF)
        dm_t = dot(wproj[...], da, NT).astype(BF)
        place(kbd, triple_t.at[t, C:2 * C])
        place(vbd, triple_t.at[t, 2 * C:3 * C])
        wide[...] = dot(dm, vbd[...]).astype(BF).astype(F32)
        dp_tail = wide[:, HEADS * LANES:]
        p_tail = prob[t, :, HEADS * LANES:]
        both_tail = dp_tail * p_tail
        sub_tail = jnp.zeros((WIN, LANES), F32)
        for h in range(HEADS):
            dp = wide[:, head_cols(h)]
            p = prob[t, :, head_cols(h)]
            sub = jnp.sum(dp * p + jnp.where(segs[h], both_tail, 0.0), axis=-1, keepdims=True)
            ds = p * (dp - sub)
            dscore[pl.ds(t * HEADS + h, WIN, stride=TH), :] = ds
            dsb[0:WIN, head_cols(h)] = (ds * root).astype(BF)
            sub_tail = jnp.where(segs[h], sub, sub_tail)
        ds_tail = p_tail * (dp_tail - sub_tail)
        dsb[0:WIN, HEADS * LANES:] = (ds_tail * root).astype(BF)
        dtails[0:WIN, :] = ds_tail
        turned = jnp.transpose(dtails[...])
        for h in range(HEADS):
            picked = pl.ds(t * HEADS + h, TAIL, stride=TH)
            dtail0[picked, :] = turned[h * TAIL:(h + 1) * TAIL, 0:LANES]
            dtail1[picked, :] = turned[h * TAIL:(h + 1) * TAIL, LANES:]

        s_dt[t, 0:C, :] = dot(kbd[...], dsb[0:WIN, :], NT).astype(BF)
        for part, (left, right) in enumerate((
            (triple_t[t, 0:C], dsb[0:WIN, :]), (dm_t, probb[t])
        )):
            base = (1 + part) * C
            over_tail = dot(left, right[:, HEADS * LANES:]).astype(BF)
            for h in range(HEADS):
                own = slice(h * HEAD, (h + 1) * HEAD)
                to = slice(base + h * HEAD, base + (h + 1) * HEAD)
                s_dt[t, to, 0:LANES] = dot(left[own], right[:, head_cols(h)]).astype(BF)
                s_dt[t, to, LANES:WIN] = over_tail[own, h * TAIL:(h + 1) * TAIL]
        dn1_t = dot(wqkv[...], s_dt[t]).astype(BF)
        dn1 = dot(dn1_t, eye[...], TN) * g1
        hat1, scale1 = norm_parts(xs[rows, :])
        grad_rows[rows, :] = da.astype(F32) + norm_grad(hat1, scale1, dn1)
        return carry

    lax.fori_loop(0, 2, attend_back, 0)
    sums[0].s3()
    sums[1].s1()
    lax.fori_loop(2, 3, attend_back, 0)
    sums[0].s4()
    sums[1].s2()
    lax.fori_loop(3, TYPES, attend_back, 0)

    total = dot(s_dt[0], s_normed[0:WIN, :])
    for t in range(1, TYPES):
        total = total + dot(s_dt[t], s_normed[t * WIN:(t + 1) * WIN, :])
    total = total.astype(BF)
    front = jnp.concatenate(
        [dot(total[k * C:(k + 1) * C], eye[...], TN) for k in range(3)]
        + [dot(s_mixed[...], s_da[...], TN)], axis=1,
    )
    for b in range(6):
        packed3[b * C:(b + 1) * C, :] = front[:, b * LANES:(b + 1) * LANES].astype(BF)
    finish(packed3, ROWS[2])
    sums[0].s5()
    sums[1].s3()
    sums[2].s0()

    for z in range(Z):
        for a in range(LAT):
            k = z * LAT + a
            base = (a // WLAT) * WIN + z * WLAT * WLON + (a % WLAT) * WLON
            rows_in[HALF * k:HALF * k + HALF, :] = grad_rows[base + HALF:base + WLON, :]
            xs[WLON * k + HALF:WLON * k + WLON, :] = grad_rows[base:base + HALF, :]
    fgrad_out[...] = rows_in[0:Z * LAT * HALF, :].astype(BF)
    edges.append(edge(3, fgrad_out, fgrad_in, east_of))

    s_table[...] = jnp.zeros_like(s_table)

    def added(blocks):
        lefts, hots = [], []
        for digit, hot, ds in blocks:
            hots.append(hot)
            lefts.append(jnp.concatenate(
                [jnp.where(digit == d, ds, 0.0) for d in range(DIGITS)], axis=0
            ).astype(BF))
        s_table[...] += dot(
            jnp.concatenate(lefts, axis=1), jnp.concatenate(hots, axis=1), NT
        )

    def main_table(step, carry):
        blocks = []
        for u in range(UNROLL):
            pair = step * UNROLL + u
            ds = jnp.concatenate(
                [dscore[th_rows(2 * pair), :], dscore[th_rows(2 * pair + 1), :]], axis=1
            )
            blocks.append(main_position(pair) + (ds,))
        added(blocks)
        return carry

    def tail_table(step, carry):
        blocks = []
        for u in range(UNROLL):
            key = step * UNROLL + u
            ds = jnp.concatenate([dtail0[th_rows(key), :], dtail1[th_rows(key), :]], axis=1)
            blocks.append(tail_position(key) + (ds,))
        added(blocks)
        return carry

    steps = WIN // 2 // UNROLL
    lax.fori_loop(0, steps // 2, main_table, 0)
    sums[0].s6()
    sums[1].s4()
    sums[2].s1()
    lax.fori_loop(steps // 2, steps, main_table, 0)
    sums[1].s5()
    sums[2].s2()
    lax.fori_loop(0, TAIL // UNROLL, tail_table, 0)
    for b in range(2):
        start = b * DIGITS * TH
        packed4[start:start + DIGITS * TH, :] = s_table[:, b * LANES:(b + 1) * LANES].astype(BF)
    finish(packed4, ROWS[3])
    sums[3].s0()
    sums[2].s3()

    edges[2].wait_recv()
    cts[0:Z * LAT // 2 * 3, :] = merged_in[...].astype(F32)
    for z in range(Z):
        for a in range(LAT // 2):
            k = z * (LAT // 2) + a
            ct_rows[8 * k:8 * k + 3, :] = cts[3 * k:3 * k + 3, :]
            merged_ref[z, a] = ct_rows[8 * k:8 * k + 6, :].astype(BF)
    sums[3].s1()
    sums[2].s4()
    edges[3].wait_recv()
    rows_in[0:Z * LAT * HALF, :] = fgrad_in[...].astype(F32)
    for z in range(Z):
        for a in range(LAT):
            k = z * LAT + a
            xs[WLON * k:WLON * k + HALF, :] = rows_in[HALF * k:HALF * k + HALF, :]
            fgrad_ref[z, a] = xs[WLON * k:WLON * k + WLON, :].astype(BF)
    sums[3].s2()
    sums[2].s5()
    sums[1].s6()
    sums[3].s3()
    sums[2].s6()
    sums[3].s4()
    sums[3].s5()
    sums[3].s6()
    for made in edges:
        made.wait_send()


def unpack_kernel(
    factor, merged_in, fgrad_in, sum1, sum2, sum3, sum4,
    merged_hbm, fgrad_hbm, qkv_hbm, proj_hbm, up_hbm, down_hbm, merge_hbm, table_hbm,
    qkv, proj, up, down, merge, table, sem,
):
    started = []

    def out(src, dst):
        made = pltpu.make_async_copy(src, dst, sem.at[len(started)])
        made.start()
        started.append(made)

    out(merged_in, merged_hbm)
    out(fgrad_in, fgrad_hbm)

    def scaled(ref, start, rows):
        return ref[start:start + rows, :].astype(F32) * factor

    for b in range(3):
        merge[:, b * LANES:(b + 1) * LANES] = scaled(sum1, b * 4 * C, 4 * C)
    out(merge, merge_hbm)
    down[:, 0:LANES] = scaled(sum2, 0, MLP)
    rest = scaled(sum2, MLP, MLP // 2)
    down[0:MLP // 2, LANES:] = rest[:, 0:C - LANES]
    down[MLP // 2:, LANES:] = rest[:, C - LANES:]
    out(down, down_hbm)
    for b in range(6):
        up[:, b * LANES:(b + 1) * LANES] = scaled(sum2, 6 * C + b * C, C)
    out(up, up_hbm)
    front = jnp.concatenate([scaled(sum3, b * C, C) for b in range(6)], axis=1)
    qkv[...] = front[:, :3 * C]
    out(qkv, qkv_hbm)
    proj[...] = front[:, 3 * C:]
    out(proj, proj_hbm)
    for b in range(2):
        for d in range(DIGITS):
            at = d * RADIX + b * LANES
            width = min(LANES, BPOS - at)
            block = scaled(sum4, (b * DIGITS + d) * TH, TH)
            for t in range(TYPES):
                table[t, :, at:at + width] = block[t * HEADS:(t + 1) * HEADS, :width]
    out(table, table_hbm)
    for made in started:
        made.wait()


def group_order():
    order = np.zeros((4 * GPAD, WIN), np.float32)
    for pa in range(2):
        for pb in range(2):
            for z in range(WZ):
                for a in range(WLAT // 2):
                    for b in range(WLON // 2):
                        cell = (z * (WLAT // 2) + a) * (WLON // 2) + b
                        token = (z * WLAT + 2 * a + pa) * WLON + 2 * b + pb
                        order[(2 * pa + pb) * GPAD + cell, token] = 1.0
    return jnp.asarray(order, BF)


def local(
    fields, norm_gain, qkv_weight, proj_weight, bias_table, bias_index, region_ids,
    mlp_gain, up_weight, down_weight, merge_gain, merge_weight, cotangent,
):
    n = lax.axis_size("lon")
    assert fields.shape[2] == WLON
    slow, fast = grid_sides(n)
    rows_of = piece_rows(n)
    gains = jnp.concatenate([norm_gain, mlp_gain, merge_gain]).reshape(6, C)
    tail_index = jnp.pad(
        bias_index[:, LANES:].T, ((0, 0), (0, RADIX - WIN)), constant_values=-1
    )
    labels = region_ids.reshape(WZ, TYPES, WLAT).transpose(1, 0, 2).reshape(TYPES, WZ * WLAT)
    labels = jnp.repeat(labels, WLON, axis=1)
    label_q = jnp.pad(labels, ((0, 0), (0, RADIX - WIN)), constant_values=-1)
    label_k = jnp.concatenate(
        [labels[:, :LANES]] + [labels[:, LANES:]] * HEADS
        + [jnp.full((TYPES, LANES - HEADS * TAIL), -2, labels.dtype)], axis=1,
    )
    labels = jnp.concatenate([label_q, label_k], axis=0)

    copies = 2 + 2 * (fast - 1) + 2 * (slow - 1)
    sums_scratch = [pltpu.VMEM((r, LANES), BF) for r in rows_of]
    sums_scratch += [pltpu.VMEM((r // 2, LANES), BF) for r in rows_of]
    sums_scratch += [pltpu.VMEM((r // 2, LANES), BF) for r in rows_of]
    sums_scratch += [pltpu.VMEM((fast - 1, r // (2 * fast), LANES), BF) for r in rows_of]
    sums_scratch += [pltpu.VMEM((r // (2 * fast), LANES), BF) for r in rows_of]
    sums_scratch += [pltpu.VMEM((slow - 1, r // n, LANES), BF) for r in rows_of]
    sums_scratch += [pltpu.SemaphoreType.DMA((copies,))] * 8
    halves = Z * LAT * HALF
    quarters = Z * LAT // 2 * 3
    outs = pl.pallas_call(
        functools.partial(block_kernel, n),
        out_shape=(
            jax.ShapeDtypeStruct(cotangent.shape, BF),
            jax.ShapeDtypeStruct(fields.shape, BF),
        ) + tuple(jax.ShapeDtypeStruct((r, LANES), BF) for r in rows_of),
        in_specs=[VMEM] * 4 + [ANY] * 9,
        out_specs=(VMEM,) * 6,
        scratch_shapes=[
            pltpu.VMEM(fields.shape, BF),
            pltpu.VMEM((Z, LAT, 8, C), BF),
            pltpu.VMEM(cotangent.shape, BF),
            pltpu.VMEM(cotangent.shape, BF),
            pltpu.VMEM(bias_table.shape, F32),
            pltpu.VMEM(bias_index.shape, jnp.int32),
            pltpu.VMEM(qkv_weight.shape, BF),
            pltpu.VMEM(proj_weight.shape, BF),
            pltpu.VMEM(up_weight.shape, BF),
            pltpu.VMEM(down_weight.shape, BF),
            pltpu.VMEM(merge_weight.shape, BF),
            pltpu.SemaphoreType.DMA((9,)),
            pltpu.SemaphoreType.DMA((4,)),
            pltpu.SemaphoreType.DMA((4,)),
            pltpu.VMEM((quarters, 2 * C), BF),
            pltpu.VMEM((quarters, 2 * C), BF),
            pltpu.VMEM((halves, C), BF),
            pltpu.VMEM((halves, C), BF),
        ] + sums_scratch + [
            pltpu.VMEM((WIN, LANES), jnp.int32),
            pltpu.VMEM((Z * LAT * 16, C), F32),
            pltpu.VMEM((Z * LAT // 2 * 8, 2 * C), F32),
            pltpu.VMEM((TOK, C), F32),
            pltpu.VMEM((TYPES * GPAD, 2 * C), F32),
            pltpu.VMEM((DIGITS * TH, RADIX), F32),
            pltpu.VMEM((3 * C, C), BF),
            pltpu.VMEM((WIN * TH, LANES), F32),
            pltpu.VMEM((TAIL * TH, LANES), F32),
            pltpu.VMEM((TAIL * TH, LANES), F32),
            pltpu.VMEM((LANES, RADIX), F32),
            pltpu.VMEM((C, C), BF),
            pltpu.VMEM((C, WIDE), BF),
            pltpu.VMEM((C, WIDE), BF),
            pltpu.VMEM((WIDE, C), BF),
            pltpu.VMEM((WIN, WIDE), F32),
            pltpu.VMEM((TYPES, WIN, WIDE), F32),
            pltpu.VMEM((TYPES, WIN, WIDE), BF),
            pltpu.VMEM((DIGITS * TH, WIDE), BF),
            pltpu.VMEM((WIN * TH, LANES), F32),
            pltpu.VMEM((TAIL * TH, LANES), F32),
            pltpu.VMEM((TAIL * TH, LANES), F32),
            pltpu.VMEM((RADIX, LANES), F32),
            pltpu.VMEM((TYPES, 3 * C, WIN), BF),
            pltpu.VMEM((TOK, C), BF),
            pltpu.VMEM((TOK, C), BF),
            pltpu.VMEM((TOK, C), BF),
            pltpu.VMEM((TOK, C), BF),
            pltpu.VMEM((TOK, MLP), F32),
            pltpu.VMEM((TOK, MLP), BF),
            pltpu.VMEM((TOK, C), BF),
            pltpu.VMEM((4, TYPES * GPAD, C), BF),
            pltpu.VMEM((TYPES * GPAD, 2 * C), BF),
            pltpu.VMEM((TOK, MLP), BF),
            pltpu.VMEM((TOK, C), BF),
            pltpu.VMEM((TOK, C), BF),
            pltpu.VMEM((TYPES, 3 * C, WIN), BF),
            pltpu.VMEM((TOK, C), F32),
            pltpu.VMEM((TYPES * GPAD, 2 * C), F32),
            pltpu.VMEM((DIGITS * TH, RADIX), F32),
        ],
        compiler_params=pltpu.CompilerParams(
            collective_id=0, has_side_effects=True, vmem_limit_bytes=56 << 20
        ),
        cost_estimate=pl.CostEstimate(
            flops=30_000_000_000, bytes_accessed=8 << 20, transcendentals=2_000_000
        ),
        name="block",
    )(
        gains, tail_index, labels, group_order(),
        fields, cotangent, bias_table, bias_index, qkv_weight, proj_weight,
        up_weight, down_weight, merge_weight,
    )

    factor = float(Z * LAT * fields.shape[2] * n) ** (-0.5)
    shapes = ((C, 3 * C), (C, C), (C, MLP), (MLP, C), (4 * C, 2 * C), (TYPES, HEADS, BPOS))
    return pl.pallas_call(
        functools.partial(unpack_kernel, factor),
        out_shape=(
            jax.ShapeDtypeStruct(cotangent.shape, BF),
            jax.ShapeDtypeStruct(fields.shape, BF),
        ) + tuple(jax.ShapeDtypeStruct(s, F32) for s in shapes),
        in_specs=[VMEM] * 6,
        out_specs=(ANY,) * 8,
        scratch_shapes=[pltpu.VMEM(s, F32) for s in shapes] + [pltpu.SemaphoreType.DMA((8,))],
        compiler_params=pltpu.CompilerParams(vmem_limit_bytes=16 << 20),
        cost_estimate=pl.CostEstimate(
            flops=1_000_000_000, bytes_accessed=6 << 20, transcendentals=0
        ),
        name="unpack",
    )(*outs)


def solution(mesh):
    grid = P("groups", None, "lon", None)
    rows = P("groups", None)
    return jax.shard_map(
        local,
        mesh=mesh,
        in_specs=(grid,) + (P(),) * 11 + (grid,),
        out_specs=(grid, grid) + (rows,) * 5 + (P("groups", None, None),),
        check_vma=False,
    )
```
